32 devices in a mesh: section: 4 (over y, x), seq: 8 (over z, core).
Axes of the slice: x: 2, y: 2, z: 4, core: 2. Of those that a mesh axis runs over, the one named last changes fastest.
Arguments:
- stream: bfloat16 [4, 1024, 4096], P('section', 'seq'), may hold values from -4 to 4
- queries: bfloat16 [4, 1024, 4096], P('section', 'seq')
- span_kv: bfloat16 [4, 2, 1024, 512], P('section', None, 'seq')
- cache_kv: bfloat16 [4, 2, 1024, 512], P('section', None, 'seq'), may hold values from -6 to 6
- cache_len: int32 [8], replicated, may hold values from 48 to 80, as said below
- context_start: int32 [1], replicated, may hold values from 1 to 1024
- block_table: int32 [8, 8], replicated, may hold values from 0 to 1, as said below
Outputs:
- handed: bfloat16 [4, 1024, 4096], P('section', 'seq')
The draws below stay inside these ranges and needn't reach their ends.
Inputs may be any that keep to these rules, and one draw needn't show every extreme that they name: `cache_len`: some index holds exactly 80 live slots. `block_table`: the diagonal is 1 and every entry above it is 0.
All inputs are finite; a program needn't handle non-finite values.
Results may differ from the reference program's by a relative error of at most 0.006.
Values may be sent and summed in bfloat16 or wider, within the bound.
A program may use at most 64 MiB of HBM per device.

```python
import math
import jax
import jax.numpy as jnp
from jax import lax

HEAD_DIM = 128
HEADS = 32
KV_HEADS = 4
TOK_DEV = 128
CACHE_DEV = 128
GROUP = 8
LIVE_MAX = 80
TOKENS = 1024
CACHE = 1024
N_SECTION = 4
N_SEQ = 8


def shaped_pairs(key):
    base = jax.random.normal(jax.random.fold_in(key, 11), (N_SECTION, 2, TOKENS, KV_HEADS * HEAD_DIM), jnp.float32)
    return base


def draw_span_kv(key, part):
    return shaped_pairs(key).astype(jnp.bfloat16)


def draw_queries(key, part):
    noise = 2.0 * jax.random.normal(jax.random.fold_in(key, 12), (N_SECTION, TOKENS, HEADS * HEAD_DIM), jnp.float32)
    return noise.astype(jnp.bfloat16)


def draw_cache_len(key, part):
    counts = jax.random.randint(jax.random.fold_in(key, 21), (N_SEQ,), 3 * LIVE_MAX // 5, LIVE_MAX + 1)
    fullest = jax.random.randint(jax.random.fold_in(key, 22), (), 0, N_SEQ)
    return jnp.where(jnp.arange(N_SEQ) == fullest, LIVE_MAX, counts).astype(jnp.int32)


def draw_block_table(key, part):
    coins = jax.random.randint(jax.random.fold_in(key, 31), (N_SEQ, N_SEQ), 0, 4)
    row_ids = jnp.arange(N_SEQ)[:, None]
    col_ids = jnp.arange(N_SEQ)[None, :]
    lower = jnp.where(coins > 0, 1, 0)
    return jnp.where(col_ids < row_ids, lower, jnp.where(col_ids == row_ids, 1, 0)).astype(jnp.int32)


def level_of(key, shape, shards, smallest, high):
    gain = 1.0
    for position, blocks in shards:
        draws = jax.random.uniform(jax.random.fold_in(jax.random.fold_in(key, 6), position), (blocks,), jnp.float32, smallest / len(shards), high / len(shards))
        gain = gain * jnp.repeat(jnp.exp(draws), shape[position] // blocks).reshape((-1,) + (1,) * (len(shape) - 1 - position))
    return gain


def bell_draw(own_key, extent, width, most, split=(), held_as=jnp.bfloat16):
    array = width * jax.random.normal(own_key, extent, jnp.float32)
    if split:
        array = array * level_of(own_key, extent, split, -0.22, 0.18)
    return jnp.clip(array, -most, most).astype(held_as)


def setup_inputs(seed: int = 0) -> dict:
    streams_of = jax.random.split(jax.random.key(seed), 8)
    return {
        "stream": bell_draw(streams_of[0], (N_SECTION, TOKENS, HEADS * HEAD_DIM), 0.5, 4.0, ((0, 4), (1, 8))),
        "queries": draw_queries(jax.random.fold_in(streams_of[7], 71), 0),
        "span_kv": draw_span_kv(jax.random.fold_in(streams_of[7], 71), 0),
        "cache_kv": bell_draw(streams_of[3], (N_SECTION, 2, CACHE, KV_HEADS * HEAD_DIM), 1.0, 6.0, ((0, 4), (2, 8))),
        "cache_len": draw_cache_len(jax.random.fold_in(streams_of[7], 71), 0),
        "context_start": jax.random.randint(streams_of[5], (1,), 1, CACHE + 1).astype(jnp.int32),
        "block_table": draw_block_table(jax.random.fold_in(streams_of[7], 71), 0),
    }


def reference(stream, queries, span_kv, cache_kv, cache_len, context_start, block_table):
    score_scale = 1.0 / math.sqrt(HEAD_DIM)
    positions = jnp.arange(CACHE, dtype=jnp.int32)
    owner = positions // CACHE_DEV
    slot_index = positions % CACHE_DEV
    cache_open = (slot_index < cache_len[owner]) & (positions >= CACHE - context_start[0])
    key_tokens = jnp.arange(TOKENS, dtype=jnp.int32)
    outputs = []
    for layer in range(N_SECTION):
        all_keys = jnp.concatenate([cache_kv[layer, 0], span_kv[layer, 0]], 0).astype(jnp.float32)
        all_keys = all_keys.reshape(CACHE + TOKENS, KV_HEADS, HEAD_DIM)
        all_values = jnp.concatenate([cache_kv[layer, 1], span_kv[layer, 1]], 0).astype(jnp.float32)
        all_values = all_values.reshape(CACHE + TOKENS, KV_HEADS, HEAD_DIM)
        layer_queries = queries[layer]

        def one_block(block):
            rows = lax.dynamic_slice_in_dim(layer_queries, block * TOK_DEV, TOK_DEV, 0).astype(jnp.float32)
            rows = rows.reshape(TOK_DEV, KV_HEADS, GROUP, HEAD_DIM)
            scores = jnp.einsum('tkgd,nkd->ktgn', rows, all_keys, precision=lax.Precision.HIGHEST) * score_scale
            query_pos = block * TOK_DEV + jnp.arange(TOK_DEV, dtype=jnp.int32)
            table_row = block_table[block]
            span_open = (key_tokens[None, :] <= query_pos[:, None]) & (table_row[key_tokens // TOK_DEV][None, :] == 1)
            allowed = jnp.concatenate([jnp.broadcast_to(cache_open[None, :], (TOK_DEV, CACHE)), span_open], 1)
            wide_mask = allowed[None, :, None, :]
            row_top = lax.optimization_barrier(jnp.max(jnp.where(wide_mask, scores, -jnp.inf), -1, keepdims=True))
            weights = jnp.where(wide_mask, jnp.exp(scores - row_top), 0.0)
            row_total = lax.optimization_barrier(jnp.sum(weights, -1))
            rounded = lax.optimization_barrier(weights.astype(jnp.bfloat16)).astype(jnp.float32)
            mixed = jnp.einsum('ktgn,nkd->ktgd', rounded, all_values, precision=lax.Precision.HIGHEST)
            mixed = mixed / row_total[..., None]
            return mixed.transpose(1, 0, 2, 3).reshape(TOK_DEV, HEADS * HEAD_DIM).astype(jnp.bfloat16)
        attn = lax.map(one_block, jnp.arange(N_SEQ, dtype=jnp.int32)).reshape(TOKENS, HEADS * HEAD_DIM)
        layer_out = (stream[layer].astype(jnp.float32) + attn.astype(jnp.float32)).astype(jnp.bfloat16)
        outputs.append(layer_out)
    return jnp.roll(jnp.stack(outputs), 1, axis=0)
```

```python
import functools
import math

import jax
import jax.numpy as jnp
from jax import lax
from jax.experimental import pallas as pl
from jax.experimental.pallas import tpu as pltpu
from jax.sharding import PartitionSpec as P

HEAD_DIM = 128
LIVE_MAX = 80
TILE_HEADS = 2
CACHE, SPAN = 0, 1
UP, DOWN, SIDE = 0, 1, 2
MESH = pl.DeviceIdType.MESH


def kernel(
    seq_count, section_count, kv_count, group_size, tok_rows, slot_rows,
    len_ref, start_ref, table_ref, stream_hbm, query_hbm, span_hbm, cache_hbm,
    out_hbm,
    cache_all, span_all, query_v, stream_v, stage, cache_scores, span_scores,
    cache_bias, span_bias, top_v, acc_v,
    local_sem, bulk_sem, send_sem, recv_sem, hand_send, hand_recv,
):
    section = lax.axis_index("section")
    me = lax.axis_index("seq")
    chip_count = seq_count // 2
    chip = me // 2
    parity = me - chip * 2
    partner = me + 1 - 2 * parity
    has_up = chip < chip_count - 1
    has_down = chip > 0
    next_section = lax.rem(section + 1, section_count)
    prev_section = lax.rem(section + section_count - 1, section_count)
    tile_cols = TILE_HEADS * HEAD_DIM
    tile_rows = TILE_HEADS * tok_rows
    tiles_per = group_size // TILE_HEADS
    pair_keys = 2 * tok_rows
    cache_rows = seq_count * LIVE_MAX
    cache_chunk = math.gcd(seq_count, 8) * LIVE_MAX
    cache_chunks = cache_rows // cache_chunk

    def piece(kind, head, shard):
        if kind == CACHE:
            rows = pl.ds(pl.multiple_of(shard * LIVE_MAX, 16), LIVE_MAX)
            return cache_all.at[head, :, rows, :]
        rows = pl.ds(pl.multiple_of(shard * tok_rows, 16), tok_rows)
        return span_all.at[head, :, rows, :]

    def local_copy(kind, head):
        cols = pl.ds(pl.multiple_of(head * HEAD_DIM, HEAD_DIM), HEAD_DIM)
        if kind == CACHE:
            source = cache_hbm.at[0, :, pl.ds(0, LIVE_MAX), cols]
        else:
            source = span_hbm.at[0, :, :, cols]
        return pltpu.make_async_copy(source, piece(kind, head, me), local_sem.at[kind, head])

    def link(way, kind, head, shard):
        target = {UP: me + 2, DOWN: me - 2, SIDE: partner}[way]
        ref = piece(kind, head, shard)
        return pltpu.make_async_remote_copy(
            src_ref=ref, dst_ref=ref,
            send_sem=send_sem.at[way, kind, head, shard],
            recv_sem=recv_sem.at[kind, head, shard],
            device_id={"seq": target}, device_id_type=MESH,
        )

    def hand(tile):
        cols = pl.ds(pl.multiple_of(tile * tile_cols, tile_cols), tile_cols)
        return pltpu.make_async_remote_copy(
            src_ref=stage.at[:, cols], dst_ref=out_hbm.at[0, :, cols],
            send_sem=hand_send.at[tile], recv_sem=hand_recv.at[tile],
            device_id={"section": next_section}, device_id_type=MESH,
        )

    for head in range(kv_count):
        local_copy(CACHE, head).start()
        local_copy(SPAN, head).start()
    query_copy = pltpu.make_async_copy(query_hbm.at[0], query_v, bulk_sem.at[0])
    stream_copy = pltpu.make_async_copy(stream_hbm.at[0], stream_v, bulk_sem.at[1])
    query_copy.start()
    stream_copy.start()

    barrier = pltpu.get_barrier_semaphore()

    def greet(device):
        pl.semaphore_signal(barrier, inc=1, device_id=device, device_id_type=MESH)

    greet({"seq": partner})
    greet({"section": next_section})
    greet({"section": prev_section})

    @pl.when(has_up)
    def _():
        greet({"seq": me + 2})

    @pl.when(has_down)
    def _():
        greet({"seq": me - 2})

    key_col = lax.broadcasted_iota(jnp.int32, (1, cache_rows), 1)
    owner = jnp.zeros((1, cache_rows), jnp.int32)
    live = jnp.full((1, cache_rows), len_ref[0], jnp.int32)
    for shard in range(1, seq_count):
        later = key_col >= shard * LIVE_MAX
        owner = jnp.where(later, shard, owner)
        live = jnp.where(later, len_ref[shard], live)
    slot = key_col - owner * LIVE_MAX
    first_visible = slot_rows * seq_count - start_ref[0]
    cache_open = (slot < live) & (owner * slot_rows + slot >= first_visible)
    cache_bias[...] = jnp.where(cache_open, 0.0, -jnp.inf).astype(jnp.float32)
    pair_col = lax.broadcasted_iota(jnp.int32, (1, pair_keys), 1)
    for pair in range(chip_count):
        hits = jnp.where(pair_col < tok_rows, table_ref[me, 2 * pair], table_ref[me, 2 * pair + 1])
        span_bias[pair, :, :] = jnp.where(hits == 1, 0.0, -jnp.inf).astype(jnp.float32)

    pl.semaphore_wait(barrier, 3 + has_up.astype(jnp.int32) + has_down.astype(jnp.int32))

    def send_own(head):
        local_copy(CACHE, head).wait()
        local_copy(SPAN, head).wait()

        @pl.when(has_up)
        def _():
            link(UP, CACHE, head, me).start()
            link(UP, SPAN, head, me).start()

        @pl.when(has_down)
        def _():
            link(DOWN, CACHE, head, me).start()

        link(SIDE, CACHE, head, me).start()
        link(SIDE, SPAN, head, me).start()

    def relay(head):
        @pl.loop(1, chip_count)
        def _(step):
            @pl.when(step <= chip)
            def _():
                shard = me - 2 * step
                for kind in (CACHE, SPAN):
                    link(UP, kind, head, shard).wait_recv()

                    @pl.when(has_up)
                    def _():
                        link(UP, kind, head, shard).start()

                    link(SIDE, kind, head, shard).start()

            @pl.when(chip + step < chip_count)
            def _():
                shard = me + 2 * step
                link(DOWN, CACHE, head, shard).wait_recv()

                @pl.when(has_down)
                def _():
                    link(DOWN, CACHE, head, shard).start()

                link(SIDE, CACHE, head, shard).start()

    def from_partner(head):
        @pl.loop(0, chip_count)
        def _(other):
            shard = partner + 2 * (other - chip)
            link(SIDE, CACHE, head, shard).wait_recv()

            @pl.when(other <= chip)
            def _():
                link(SIDE, SPAN, head, shard).wait_recv()

    factor = math.log2(math.e) / math.sqrt(HEAD_DIM)

    def query_key(rows, keys):
        return lax.dot_general(
            rows, keys, (((1,), (1,)), ((), ())), preferred_element_type=jnp.float32
        )

    def lane_top(scores):
        best = scores[:, :HEAD_DIM]
        for first in range(HEAD_DIM, scores.shape[1], HEAD_DIM):
            best = jnp.maximum(best, scores[:, first : first + HEAD_DIM])
        return best

    def weighted(scores, row_top, values):
        weights = jnp.exp2((scores - row_top) * factor).astype(jnp.bfloat16)
        wide = jnp.concatenate([values, jnp.ones_like(values)], axis=1)
        return jnp.dot(weights, wide, preferred_element_type=jnp.float32)

    def cache_part(chunk):
        return pl.ds(pl.multiple_of(chunk * cache_chunk, 16), cache_chunk)

    def cache_lanes(chunk):
        if cache_chunks == 1:
            return pl.ds(0, cache_chunk)
        return pl.ds(pl.multiple_of(chunk * cache_chunk, HEAD_DIM), cache_chunk)

    def span_part(pair):
        return pl.ds(pl.multiple_of(pair * pair_keys, HEAD_DIM), pair_keys)

    def attend(head, tile):
        def cols(index):
            return pl.ds(pl.multiple_of((tile * TILE_HEADS + index) * HEAD_DIM, HEAD_DIM), HEAD_DIM)

        rows = jnp.concatenate([query_v[:, cols(i)] for i in range(TILE_HEADS)], axis=0)
        scores = query_key(rows, span_all[head, 0, span_part(chip), :]) + span_bias[chip]
        token = lax.broadcasted_iota(jnp.int32, (tok_rows, pair_keys), 0) + parity * tok_rows
        key = lax.broadcasted_iota(jnp.int32, (tok_rows, pair_keys), 1)
        causal = jnp.concatenate([key <= token] * TILE_HEADS, axis=0)
        scores = jnp.where(causal, scores, -jnp.inf)
        span_scores[:, span_part(chip)] = scores
        top_v[...] = lane_top(scores)

        def span_scored(pair, _):
            scores = query_key(rows, span_all[head, 0, span_part(pair), :]) + span_bias[pair]
            span_scores[:, span_part(pair)] = scores
            top_v[...] = jnp.maximum(top_v[...], lane_top(scores))
            return 0

        def cache_scored(chunk, _):
            scores = query_key(rows, cache_all[head, 0, cache_part(chunk), :])
            scores = scores + cache_bias[:, cache_lanes(chunk)]
            cache_scores[:, cache_lanes(chunk)] = scores
            top_v[...] = jnp.maximum(top_v[...], lane_top(scores))
            return 0

        lax.fori_loop(0, cache_chunks, cache_scored, 0)
        lax.fori_loop(0, chip, span_scored, 0)
        row_top = jnp.max(top_v[...], axis=1, keepdims=True)

        def cache_mixed(chunk, _):
            acc_v[...] += weighted(
                cache_scores[:, cache_lanes(chunk)], row_top, cache_all[head, 1, cache_part(chunk), :]
            )
            return 0

        def span_mixed(pair, _):
            acc_v[...] += weighted(
                span_scores[:, span_part(pair)], row_top, span_all[head, 1, span_part(pair), :]
            )
            return 0

        acc_v[...] = weighted(
            cache_scores[:, cache_lanes(0)], row_top, cache_all[head, 1, cache_part(0), :]
        )
        if cache_chunks > 1:
            lax.fori_loop(1, cache_chunks, cache_mixed, 0)
        lax.fori_loop(0, chip + 1, span_mixed, 0)
        attn = (acc_v[:, :HEAD_DIM] / acc_v[:, HEAD_DIM:]).astype(jnp.bfloat16).astype(jnp.float32)
        for index in range(TILE_HEADS):
            mixed = attn[index * tok_rows : (index + 1) * tok_rows]
            total = stream_v[:, cols(index)].astype(jnp.float32) + mixed
            stage[:, cols(index)] = total.astype(jnp.bfloat16)

    send_own(0)
    send_own(1)
    query_copy.wait()
    stream_copy.wait()

    @pl.loop(0, kv_count)
    def _(head):
        relay(head)

        @pl.when(head + 2 < kv_count)
        def _():
            send_own(head + 2)

        from_partner(head)

        @pl.loop(0, tiles_per)
        def _(part):
            tile = head * tiles_per + part
            attend(head, tile)

            @pl.when(tile > 0)
            def _():
                hand(tile - 1).start()

    @pl.loop(0, kv_count)
    def _(head):
        @pl.loop(0, chip_count)
        def _(other):
            shard = parity + 2 * other
            link(SIDE, CACHE, head, shard).wait_send()

            @pl.when(other <= chip)
            def _():
                link(SIDE, SPAN, head, shard).wait_send()

                @pl.when(has_up)
                def _():
                    link(UP, CACHE, head, shard).wait_send()
                    link(UP, SPAN, head, shard).wait_send()

            @pl.when((other >= chip) & has_down)
            def _():
                link(DOWN, CACHE, head, shard).wait_send()

    tile_count = kv_count * tiles_per
    hand(tile_count - 1).start()

    @pl.loop(0, tile_count)
    def _(tile):
        hand(tile).wait_recv()
        hand(tile).wait_send()


def shards(stream, queries, span_kv, cache_kv, cache_len, context_start, block_table):
    seq_count = lax.axis_size("seq")
    section_count = lax.axis_size("section")
    tok_rows, query_width = queries.shape[1:]
    key_width = span_kv.shape[3]
    kv_count = key_width // HEAD_DIM
    group_size = query_width // key_width
    slot_rows = cache_kv.shape[2]
    tile_rows = TILE_HEADS * tok_rows
    tile_count = kv_count * group_size // TILE_HEADS
    smem = pl.BlockSpec(memory_space=pltpu.SMEM)
    hbm = pl.BlockSpec(memory_space=pl.ANY)
    bf16, f32 = jnp.bfloat16, jnp.float32
    return pl.pallas_call(
        functools.partial(
            kernel, seq_count, section_count, kv_count, group_size, tok_rows, slot_rows
        ),
        out_shape=jax.ShapeDtypeStruct(stream.shape, bf16),
        in_specs=[smem] * 3 + [hbm] * 4,
        out_specs=hbm,
        scratch_shapes=[
            pltpu.VMEM((kv_count, 2, seq_count * LIVE_MAX, HEAD_DIM), bf16),
            pltpu.VMEM((kv_count, 2, seq_count * tok_rows, HEAD_DIM), bf16),
            pltpu.VMEM((tok_rows, query_width), bf16),
            pltpu.VMEM((tok_rows, query_width), bf16),
            pltpu.VMEM((tok_rows, query_width), bf16),
            pltpu.VMEM((tile_rows, seq_count * LIVE_MAX), f32),
            pltpu.VMEM((tile_rows, seq_count * tok_rows), f32),
            pltpu.VMEM((1, seq_count * LIVE_MAX), f32),
            pltpu.VMEM((seq_count // 2, 1, 2 * tok_rows), f32),
            pltpu.VMEM((tile_rows, HEAD_DIM), f32),
            pltpu.VMEM((tile_rows, 2 * HEAD_DIM), f32),
            pltpu.SemaphoreType.DMA((2, kv_count)),
            pltpu.SemaphoreType.DMA((2,)),
            pltpu.SemaphoreType.DMA((3, 2, kv_count, seq_count)),
            pltpu.SemaphoreType.DMA((2, kv_count, seq_count)),
            pltpu.SemaphoreType.DMA((tile_count,)),
            pltpu.SemaphoreType.DMA((tile_count,)),
        ],
        compiler_params=pltpu.CompilerParams(collective_id=0, has_side_effects=True),
    )(cache_len, context_start, block_table, stream, queries, span_kv, cache_kv)


def solution(mesh):
    return jax.shard_map(
        shards,
        mesh=mesh,
        in_specs=(
            P("section", "seq", None),
            P("section", "seq", None),
            P("section", None, "seq", None),
            P("section", None, "seq", None),
            P(),
            P(),
            P(),
        ),
        out_specs=P("section", "seq", None),
        check_vma=False,
    )
```

```python
import functools
import math

import jax
import jax.numpy as jnp
from jax import lax
from jax.experimental import pallas as pl
from jax.experimental.pallas import tpu as pltpu
from jax.sharding import PartitionSpec as P

HEAD_DIM = 128
LIVE_MAX = 80
TILE_HEADS = 2
BLOCK_HEADS = 8
CACHE, SPAN = 0, 1
UP, DOWN, SIDE = 0, 1, 2
MESH = pl.DeviceIdType.MESH


def kernel(
    seq_count, section_count, kv_count, group_size, tok_rows, slot_rows,
    len_ref, start_ref, table_ref, stream_hbm, query_hbm, span_hbm, cache_hbm,
    out_hbm,
    cache_all, span_all, query_v, stream_v, stage, cache_scores, span_scores,
    cache_bias, span_bias, top_v, acc_v,
    local_sem, bulk_sem, send_sem, recv_sem, hand_send, hand_recv,
):
    section = lax.axis_index("section")
    me = lax.axis_index("seq")
    chip_count = seq_count // 2
    chip = me // 2
    parity = me - chip * 2
    partner = me + 1 - 2 * parity
    has_up = chip < chip_count - 1
    has_down = chip > 0
    next_section = lax.rem(section + 1, section_count)
    prev_section = lax.rem(section + section_count - 1, section_count)
    tile_cols = TILE_HEADS * HEAD_DIM
    tiles_per = BLOCK_HEADS // TILE_HEADS
    blocks_per = group_size // BLOCK_HEADS
    pair_keys = 2 * tok_rows
    cache_rows = seq_count * LIVE_MAX
    cache_chunk = math.gcd(seq_count, 8) * LIVE_MAX
    cache_chunks = cache_rows // cache_chunk

    def piece(kind, head, shard):
        if kind == CACHE:
            rows = pl.ds(pl.multiple_of(shard * LIVE_MAX, 16), LIVE_MAX)
            return cache_all.at[head, :, rows, :]
        rows = pl.ds(pl.multiple_of(shard * tok_rows, 16), tok_rows)
        return span_all.at[head, :, rows, :]

    def local_copy(kind, head):
        cols = pl.ds(pl.multiple_of(head * HEAD_DIM, HEAD_DIM), HEAD_DIM)
        if kind == CACHE:
            source = cache_hbm.at[0, :, pl.ds(0, LIVE_MAX), cols]
        else:
            source = span_hbm.at[0, :, :, cols]
        return pltpu.make_async_copy(source, piece(kind, head, me), local_sem.at[kind, head])

    def link(way, kind, head, shard):
        target = {UP: me + 2, DOWN: me - 2, SIDE: partner}[way]
        ref = piece(kind, head, shard)
        return pltpu.make_async_remote_copy(
            src_ref=ref, dst_ref=ref,
            send_sem=send_sem.at[way, kind, head, shard],
            recv_sem=recv_sem.at[kind, head, shard],
            device_id={"seq": target}, device_id_type=MESH,
        )

    def hand(tile):
        cols = pl.ds(pl.multiple_of(tile * tile_cols, tile_cols), tile_cols)
        return pltpu.make_async_remote_copy(
            src_ref=stage.at[:, cols], dst_ref=out_hbm.at[0, :, cols],
            send_sem=hand_send.at[tile], recv_sem=hand_recv.at[tile],
            device_id={"section": next_section}, device_id_type=MESH,
        )

    for head in range(kv_count):
        local_copy(CACHE, head).start()
        local_copy(SPAN, head).start()
    query_copy = pltpu.make_async_copy(query_hbm.at[0], query_v, bulk_sem.at[0])
    stream_copy = pltpu.make_async_copy(stream_hbm.at[0], stream_v, bulk_sem.at[1])
    query_copy.start()
    stream_copy.start()

    barrier = pltpu.get_barrier_semaphore()

    def greet(device):
        pl.semaphore_signal(barrier, inc=1, device_id=device, device_id_type=MESH)

    greet({"seq": partner})
    greet({"section": next_section})
    greet({"section": prev_section})

    @pl.when(has_up)
    def _():
        greet({"seq": me + 2})

    @pl.when(has_down)
    def _():
        greet({"seq": me - 2})

    key_col = lax.broadcasted_iota(jnp.int32, (1, cache_rows), 1)
    owner = jnp.zeros((1, cache_rows), jnp.int32)
    live = jnp.full((1, cache_rows), len_ref[0], jnp.int32)
    for shard in range(1, seq_count):
        later = key_col >= shard * LIVE_MAX
        owner = jnp.where(later, shard, owner)
        live = jnp.where(later, len_ref[shard], live)
    slot = key_col - owner * LIVE_MAX
    first_visible = slot_rows * seq_count - start_ref[0]
    cache_open = (slot < live) & (owner * slot_rows + slot >= first_visible)
    cache_bias[...] = jnp.where(cache_open, 0.0, -jnp.inf).astype(jnp.float32)
    pair_col = lax.broadcasted_iota(jnp.int32, (1, pair_keys), 1)
    for pair in range(chip_count):
        hits = jnp.where(pair_col < tok_rows, table_ref[me, 2 * pair], table_ref[me, 2 * pair + 1])
        span_bias[pair, :, :] = jnp.where(hits == 1, 0.0, -jnp.inf).astype(jnp.float32)

    pl.semaphore_wait(barrier, 3 + has_up.astype(jnp.int32) + has_down.astype(jnp.int32))

    def send_own(head):
        local_copy(CACHE, head).wait()
        local_copy(SPAN, head).wait()

        @pl.when(has_up)
        def _():
            link(UP, CACHE, head, me).start()
            link(UP, SPAN, head, me).start()

        @pl.when(has_down)
        def _():
            link(DOWN, CACHE, head, me).start()

        link(SIDE, CACHE, head, me).start()
        link(SIDE, SPAN, head, me).start()

    def relay(head):
        @pl.loop(1, chip_count)
        def _(step):
            @pl.when(step <= chip)
            def _():
                shard = me - 2 * step
                for kind in (CACHE, SPAN):
                    link(UP, kind, head, shard).wait_recv()

                    @pl.when(has_up)
                    def _():
                        link(UP, kind, head, shard).start()

                    link(SIDE, kind, head, shard).start()

            @pl.when(chip + step < chip_count)
            def _():
                shard = me + 2 * step
                link(DOWN, CACHE, head, shard).wait_recv()

                @pl.when(has_down)
                def _():
                    link(DOWN, CACHE, head, shard).start()

                link(SIDE, CACHE, head, shard).start()

    def from_partner(head):
        @pl.loop(0, chip_count)
        def _(other):
            shard = partner + 2 * (other - chip)
            link(SIDE, CACHE, head, shard).wait_recv()

            @pl.when(other <= chip)
            def _():
                link(SIDE, SPAN, head, shard).wait_recv()

    factor = math.log2(math.e) / math.sqrt(HEAD_DIM)

    def query_key(rows, keys):
        return lax.dot_general(
            rows, keys, (((1,), (1,)), ((), ())), preferred_element_type=jnp.float32
        )

    def lane_top(scores):
        best = scores[:, :HEAD_DIM]
        for first in range(HEAD_DIM, scores.shape[1], HEAD_DIM):
            best = jnp.maximum(best, scores[:, first : first + HEAD_DIM])
        return best

    def weighted(scores, values):
        tops = jnp.concatenate([top_v[...]] * (scores.shape[1] // HEAD_DIM), axis=1)
        weights = jnp.exp2((scores - tops) * factor).astype(jnp.bfloat16)
        wide = jnp.concatenate([values, jnp.ones_like(values)], axis=1)
        return jnp.dot(weights, wide, preferred_element_type=jnp.float32)

    def cache_part(chunk):
        return pl.ds(pl.multiple_of(chunk * cache_chunk, 16), cache_chunk)

    def cache_lanes(chunk):
        if cache_chunks == 1:
            return pl.ds(0, cache_chunk)
        return pl.ds(pl.multiple_of(chunk * cache_chunk, HEAD_DIM), cache_chunk)

    def span_part(pair):
        return pl.ds(pl.multiple_of(pair * pair_keys, HEAD_DIM), pair_keys)

    def attend(head, block):
        def cols(index):
            first = (block * BLOCK_HEADS + index) * HEAD_DIM
            return pl.ds(pl.multiple_of(first, HEAD_DIM), HEAD_DIM)

        def rows():
            return jnp.concatenate([query_v[:, cols(i)] for i in range(BLOCK_HEADS)], axis=0)

        scores = query_key(rows(), span_all[head, 0, span_part(chip), :]) + span_bias[chip]
        token = lax.broadcasted_iota(jnp.int32, (tok_rows, pair_keys), 0) + parity * tok_rows
        key = lax.broadcasted_iota(jnp.int32, (tok_rows, pair_keys), 1)
        causal = jnp.concatenate([key <= token] * BLOCK_HEADS, axis=0)
        scores = jnp.where(causal, scores, -jnp.inf)
        span_scores[:, span_part(chip)] = scores
        top_v[...] = lane_top(scores)

        def span_scored(pair, _):
            scores = query_key(rows(), span_all[head, 0, span_part(pair), :]) + span_bias[pair]
            span_scores[:, span_part(pair)] = scores
            top_v[...] = jnp.maximum(top_v[...], lane_top(scores))
            return 0

        def cache_scored(chunk, _):
            scores = query_key(rows(), cache_all[head, 0, cache_part(chunk), :])
            scores = scores + cache_bias[:, cache_lanes(chunk)]
            cache_scores[:, cache_lanes(chunk)] = scores
            top_v[...] = jnp.maximum(top_v[...], lane_top(scores))
            return 0

        lax.fori_loop(0, cache_chunks, cache_scored, 0)
        lax.fori_loop(0, chip, span_scored, 0)
        row_top = jnp.max(top_v[...], axis=1, keepdims=True)
        top_v[...] = jnp.broadcast_to(row_top, top_v.shape)

        def cache_mixed(chunk):
            return weighted(cache_scores[:, cache_lanes(chunk)], cache_all[head, 1, cache_part(chunk), :])

        def span_mixed(pair):
            return weighted(span_scores[:, span_part(pair)], span_all[head, 1, span_part(pair), :])

        def cache_added(chunk, _):
            acc_v[...] += cache_mixed(chunk)
            return 0

        def span_added(pair, _):
            acc_v[...] += span_mixed(pair)
            return 0

        acc_v[...] = cache_mixed(0)
        if cache_chunks > 1:
            lax.fori_loop(1, cache_chunks, cache_added, 0)
        lax.fori_loop(0, chip + 1, span_added, 0)

    def finish(tile, part):
        for index in range(TILE_HEADS):
            first = pl.multiple_of((part * TILE_HEADS + index) * tok_rows, tok_rows)
            mixed = acc_v[pl.ds(first, tok_rows), :]
            attn = (mixed[:, :HEAD_DIM] / mixed[:, HEAD_DIM:]).astype(jnp.bfloat16)
            first = (tile * TILE_HEADS + index) * HEAD_DIM
            cols = pl.ds(pl.multiple_of(first, HEAD_DIM), HEAD_DIM)
            total = stream_v[:, cols].astype(jnp.float32) + attn.astype(jnp.float32)
            stage[:, cols] = total.astype(jnp.bfloat16)

    send_own(0)
    send_own(1)
    query_copy.wait()
    stream_copy.wait()

    @pl.loop(0, kv_count)
    def _(head):
        relay(head)

        @pl.when(head + 2 < kv_count)
        def _():
            send_own(head + 2)

        from_partner(head)

        @pl.loop(0, blocks_per)
        def _(inner):
            block = head * blocks_per + inner
            attend(head, block)

            @pl.loop(0, tiles_per)
            def _(part):
                tile = block * tiles_per + part
                finish(tile, part)

                @pl.when(tile > 0)
                def _():
                    hand(tile - 1).start()

    @pl.loop(0, kv_count)
    def _(head):
        @pl.loop(0, chip_count)
        def _(other):
            shard = parity + 2 * other
            link(SIDE, CACHE, head, shard).wait_send()

            @pl.when(other <= chip)
            def _():
                link(SIDE, SPAN, head, shard).wait_send()

                @pl.when(has_up)
                def _():
                    link(UP, CACHE, head, shard).wait_send()
                    link(UP, SPAN, head, shard).wait_send()

            @pl.when((other >= chip) & has_down)
            def _():
                link(DOWN, CACHE, head, shard).wait_send()

    tile_count = kv_count * group_size // TILE_HEADS
    hand(tile_count - 1).start()

    @pl.loop(0, tile_count)
    def _(tile):
        hand(tile).wait_recv()
        hand(tile).wait_send()


def shards(stream, queries, span_kv, cache_kv, cache_len, context_start, block_table):
    seq_count = lax.axis_size("seq")
    section_count = lax.axis_size("section")
    tok_rows, query_width = queries.shape[1:]
    key_width = span_kv.shape[3]
    kv_count = key_width // HEAD_DIM
    group_size = query_width // key_width
    slot_rows = cache_kv.shape[2]
    block_rows = BLOCK_HEADS * tok_rows
    tile_count = kv_count * group_size // TILE_HEADS
    smem = pl.BlockSpec(memory_space=pltpu.SMEM)
    hbm = pl.BlockSpec(memory_space=pl.ANY)
    bf16, f32 = jnp.bfloat16, jnp.float32
    return pl.pallas_call(
        functools.partial(
            kernel, seq_count, section_count, kv_count, group_size, tok_rows, slot_rows
        ),
        out_shape=jax.ShapeDtypeStruct(stream.shape, bf16),
        in_specs=[smem] * 3 + [hbm] * 4,
        out_specs=hbm,
        scratch_shapes=[
            pltpu.VMEM((kv_count, 2, seq_count * LIVE_MAX, HEAD_DIM), bf16),
            pltpu.VMEM((kv_count, 2, seq_count * tok_rows, HEAD_DIM), bf16),
            pltpu.VMEM((tok_rows, query_width), bf16),
            pltpu.VMEM((tok_rows, query_width), bf16),
            pltpu.VMEM((tok_rows, query_width), bf16),
            pltpu.VMEM((block_rows, seq_count * LIVE_MAX), f32),
            pltpu.VMEM((block_rows, seq_count * tok_rows), f32),
            pltpu.VMEM((1, seq_count * LIVE_MAX), f32),
            pltpu.VMEM((seq_count // 2, 1, 2 * tok_rows), f32),
            pltpu.VMEM((block_rows, HEAD_DIM), f32),
            pltpu.VMEM((block_rows, 2 * HEAD_DIM), f32),
            pltpu.SemaphoreType.DMA((2, kv_count)),
            pltpu.SemaphoreType.DMA((2,)),
            pltpu.SemaphoreType.DMA((3, 2, kv_count, seq_count)),
            pltpu.SemaphoreType.DMA((2, kv_count, seq_count)),
            pltpu.SemaphoreType.DMA((tile_count,)),
            pltpu.SemaphoreType.DMA((tile_count,)),
        ],
        compiler_params=pltpu.CompilerParams(collective_id=0, has_side_effects=True),
    )(cache_len, context_start, block_table, stream, queries, span_kv, cache_kv)


def solution(mesh):
    return jax.shard_map(
        shards,
        mesh=mesh,
        in_specs=(
            P("section", "seq", None),
            P("section", "seq", None),
            P("section", None, "seq", None),
            P("section", None, "seq", None),
            P(),
            P(),
            P(),
        ),
        out_specs=P("section", "seq", None),
        check_vma=False,
    )
```
